8 devices in a mesh: fsdp: 8 (over z, y, x, core).
Axes of the slice: x: 2, y: 2, z: 1, core: 2. Of those that a mesh axis runs over, the one named last changes fastest.
Arguments:
- hidden: bfloat16 [64, 512, 1536], P('fsdp')
- grad_out: bfloat16 [64, 512, 1536], P('fsdp')
- positions: int32 [64, 512], P('fsdp')
- gain_attn: bfloat16 [1536], P('fsdp')
- w_q: bfloat16 [1536, 1536], P('fsdp')
- b_q: bfloat16 [1536], P('fsdp')
- w_k: bfloat16 [1536, 256], P('fsdp')
- b_k: bfloat16 [256], P('fsdp')
- w_v: bfloat16 [1536, 256], P('fsdp')
- b_v: bfloat16 [256], P('fsdp')
- w_o: bfloat16 [1536, 1536], P('fsdp')
- gain_mlp: bfloat16 [1536], P('fsdp')
- w_gate: bfloat16 [1536, 8960], P('fsdp')
- w_up: bfloat16 [1536, 8960], P('fsdp')
- w_down: bfloat16 [8960, 1536], P('fsdp')
Outputs:
- output 1: bfloat16 [64, 512, 1536], P('fsdp')
- output 2: bfloat16 [64, 512, 1536], P('fsdp')
- output 3: float32 [1536], P('fsdp')
- output 4: float32 [1536, 1536], P('fsdp')
- output 5: float32 [1536], P('fsdp')
- output 6: float32 [1536, 256], P('fsdp')
- output 7: float32 [256], P('fsdp')
- output 8: float32 [1536, 256], P('fsdp')
- output 9: float32 [256], P('fsdp')
- output 10: float32 [1536, 1536], P('fsdp')
- output 11: float32 [1536], P('fsdp')
- output 12: float32 [1536, 8960], P('fsdp')
- output 13: float32 [1536, 8960], P('fsdp')
- output 14: float32 [8960, 1536], P('fsdp')
All inputs are finite; a program needn't handle non-finite values.
Results may differ from the reference program's by a relative error of at most 0.0163765.
Values are sent between devices in bfloat16 or wider.
A program may use at most 1 GiB of HBM per device.

```python
import math
import jax
import jax.numpy as jnp
from jax import lax

D = 1536
HEADS = 12
KV_HEADS = 2
HEAD = 128
FF = 8960
BATCH = 64
SEQ = 512
NORM_EPS = 1e-6
ROPE_THETA = 1000000.0
GROUP_SEQS = math.gcd(BATCH, max(1, 512 // SEQ))


def setup_inputs(seed: int = 0) -> dict:
    key_list = jax.random.split(jax.random.key(seed), 16)
    q_width = HEADS * HEAD
    kv_width = KV_HEADS * HEAD
    scale_d = 1.0 / math.sqrt(D)

    def normal_f32(key_index, arr_shape):
        return jax.random.normal(key_list[key_index], arr_shape, jnp.float32)

    pos_gaps = jax.random.randint(key_list[2], (BATCH, SEQ), 1, 9)
    pos_starts = jax.random.randint(key_list[3], (BATCH, 1), 0, 512)
    positions = (pos_starts + jnp.cumsum(pos_gaps, axis=1) - 1).astype(jnp.int32)
    return {
        'hidden': normal_f32(0, (BATCH, SEQ, D)).astype(jnp.bfloat16),
        'grad_out': normal_f32(1, (BATCH, SEQ, D)).astype(jnp.bfloat16),
        'positions': positions,
        'gain_attn': (1.0 + 0.3 * normal_f32(4, (D,))).astype(jnp.bfloat16),
        'w_q': (normal_f32(5, (D, q_width)) * scale_d).astype(jnp.bfloat16),
        'b_q': (0.5 * normal_f32(6, (q_width,))).astype(jnp.bfloat16),
        'w_k': (normal_f32(7, (D, kv_width)) * scale_d).astype(jnp.bfloat16),
        'b_k': normal_f32(8, (kv_width,)).astype(jnp.bfloat16),
        'w_v': (normal_f32(9, (D, kv_width)) * scale_d).astype(jnp.bfloat16),
        'b_v': (0.5 * normal_f32(10, (kv_width,))).astype(jnp.bfloat16),
        'w_o': (normal_f32(11, (q_width, D)) / math.sqrt(q_width)).astype(jnp.bfloat16),
        'gain_mlp': (1.0 + 0.3 * normal_f32(12, (D,))).astype(jnp.bfloat16),
        'w_gate': (normal_f32(13, (D, FF)) * scale_d).astype(jnp.bfloat16),
        'w_up': (normal_f32(14, (D, FF)) * scale_d).astype(jnp.bfloat16),
        'w_down': (normal_f32(15, (FF, D)) / math.sqrt(FF)).astype(jnp.bfloat16),
    }


def rope_tables(positions):
    inv_freq = 1.0 / jnp.power(ROPE_THETA, jnp.arange(0, HEAD, 2).astype(jnp.float32) / HEAD)
    angles = positions.astype(jnp.float32)[:, :, None] * inv_freq
    angles = jnp.concatenate([angles, angles], axis=-1)[:, :, None, :]
    return jnp.cos(angles), jnp.sin(angles)


def rotate_half(vec_in):
    half_dim = vec_in.shape[-1] // 2
    return jnp.concatenate([-vec_in[..., half_dim:], vec_in[..., :half_dim]], axis=-1)


def rms_norm(val_f32, gain_vec):
    inv_rms = lax.rsqrt(jnp.mean(val_f32 * val_f32, axis=-1, keepdims=True) + NORM_EPS)
    return (val_f32 * inv_rms * gain_vec).astype(jnp.bfloat16).astype(jnp.float32)


def layer_forward(params, hidden, positions):
    gain_attn, w_q, b_q, w_k, b_k, w_v, b_v, w_o, gain_mlp, w_gate, w_up, w_down = params
    n_batch = hidden.shape[0]
    q_per_kv = HEADS // KV_HEADS
    cos_t, sin_t = rope_tables(positions)
    hidden_f32 = hidden.astype(jnp.float32)
    normed_attn = rms_norm(hidden_f32, gain_attn)
    q_lin = (jnp.einsum('bsd,de->bse', normed_attn, w_q) + b_q).reshape(n_batch, SEQ, HEADS, HEAD)
    k_lin = (jnp.einsum('bsd,de->bse', normed_attn, w_k) + b_k).reshape(n_batch, SEQ, KV_HEADS, HEAD)
    v_states = (jnp.einsum('bsd,de->bse', normed_attn, w_v) + b_v).astype(jnp.bfloat16).astype(jnp.float32)
    v_states = v_states.reshape(n_batch, SEQ, KV_HEADS, HEAD)
    q_states = (q_lin * cos_t + rotate_half(q_lin) * sin_t).astype(jnp.bfloat16).astype(jnp.float32)
    q_states = q_states.reshape(n_batch, SEQ, KV_HEADS, q_per_kv, HEAD)
    k_states = (k_lin * cos_t + rotate_half(k_lin) * sin_t).astype(jnp.bfloat16).astype(jnp.float32)
    scores = jnp.einsum('bqkgd,bskd->bkgqs', q_states, k_states) / math.sqrt(HEAD)
    causal = jnp.arange(SEQ)[:, None] >= jnp.arange(SEQ)[None, :]
    attn_probs = jax.nn.softmax(jnp.where(causal, scores, -1e30), axis=-1)
    attn_probs = attn_probs.astype(jnp.bfloat16).astype(jnp.float32)
    attn_out = jnp.einsum('bkgqs,bskd->bqkgd', attn_probs, v_states).astype(jnp.bfloat16).astype(jnp.float32)
    attn_out = attn_out.reshape(n_batch, SEQ, HEADS * HEAD)
    resid_mid = (hidden_f32 + jnp.einsum('bse,ed->bsd', attn_out, w_o)).astype(jnp.bfloat16).astype(jnp.float32)
    normed_mlp = rms_norm(resid_mid, gain_mlp)
    gate_pre = jnp.einsum('bsd,df->bsf', normed_mlp, w_gate)
    up_proj = jnp.einsum('bsd,df->bsf', normed_mlp, w_up)
    act_mlp = (jax.nn.silu(gate_pre) * up_proj).astype(jnp.bfloat16).astype(jnp.float32)
    return (resid_mid + jnp.einsum('bsf,fd->bsd', act_mlp, w_down)).astype(jnp.bfloat16)


def reference(hidden, grad_out, positions, gain_attn, w_q, b_q, w_k, b_k, w_v, b_v, w_o, gain_mlp, w_gate, w_up, w_down):
    params = tuple(weight_arr.astype(jnp.float32) for weight_arr in (gain_attn, w_q, b_q, w_k, b_k, w_v, b_v, w_o, gain_mlp, w_gate, w_up, w_down))
    n_steps = BATCH // GROUP_SEQS

    def scan_body(grad_acc, step_in):
        hid_step, gout_step, pos_step = step_in

        def forward_only(param_list, hid_in):
            return layer_forward(param_list, hid_in, pos_step)

        layer_out, pullback = jax.vjp(forward_only, params, hid_step)
        d_params, d_hidden = pullback(gout_step)
        return jax.tree.map(jnp.add, grad_acc, d_params), (layer_out, d_hidden)

    step_inputs = (
        hidden.reshape(n_steps, GROUP_SEQS, SEQ, D),
        grad_out.reshape(n_steps, GROUP_SEQS, SEQ, D),
        positions.reshape(n_steps, GROUP_SEQS, SEQ),
    )
    grad_init = jax.tree.map(jnp.zeros_like, params)
    grad_sum, (out_steps, dx_steps) = lax.scan(scan_body, grad_init, step_inputs)
    return (out_steps.reshape(BATCH, SEQ, D), dx_steps.reshape(BATCH, SEQ, D), grad_sum[0], grad_sum[1], grad_sum[2], grad_sum[3], grad_sum[4], grad_sum[5], grad_sum[6], grad_sum[7], grad_sum[8], grad_sum[9], grad_sum[10], grad_sum[11])
```

```python
import functools
import math
import jax
import jax.numpy as jnp
from jax import lax
from jax.experimental import pallas as pl
from jax.experimental.pallas import tpu as pltpu
from jax.sharding import PartitionSpec as P

HEAD_DIM = 128
NORM_EPS = 1e-6
ROPE_THETA = 1000000.0
FSDP_AXIS = 'fsdp'
LOG2E = 1.4426950408889634
Q_BLK = 256
NT = (((1,), (1,)), ((), ()))
NN = (((1,), (0,)), ((), ()))


def matmul_f32(eq_form, lhs_arr, rhs_arr):
    return jnp.einsum(eq_form, lhs_arr, rhs_arr, preferred_element_type=jnp.float32)


def dot_f32(lhs_arr, rhs_arr, dims):
    return lax.dot_general(lhs_arr, rhs_arr, dims, preferred_element_type=jnp.float32)


def rope_tables(positions):
    inv_freq = 1.0 / jnp.power(ROPE_THETA, jnp.arange(0, HEAD_DIM, 2).astype(jnp.float32) / HEAD_DIM)
    angles = positions.astype(jnp.float32).reshape(-1, 1) * inv_freq
    cos_h, sin_h = jnp.cos(angles), jnp.sin(angles)
    return jnp.concatenate([cos_h, cos_h], axis=-1), jnp.concatenate([-sin_h, sin_h], axis=-1)


def causal_keep(n_blk):
    key_i = lax.broadcasted_iota(jnp.int32, (n_blk, n_blk), 0)
    qry_i = lax.broadcasted_iota(jnp.int32, (n_blk, n_blk), 1)
    return key_i <= qry_i


def attn_fwd_kernel(n_group, q_ref, k_ref, v_ref, cos_ref, sin_ref, o_ref, qr_ref, kr_ref, vb_ref, lse_ref):
    n_seq = k_ref.shape[0]
    cos_t, sin_t = cos_ref[...], sin_ref[...]
    score_mul = LOG2E / math.sqrt(HEAD_DIM)
    keep = causal_keep(Q_BLK)

    def rope(vec_in):
        return (vec_in * cos_t + pltpu.roll(vec_in, HEAD_DIM // 2, 1) * sin_t).astype(jnp.bfloat16)

    kr_ref[...] = rope(k_ref[...])
    v_f32 = v_ref[...].astype(jnp.bfloat16).astype(jnp.float32)
    vb_ref[...] = v_f32.astype(jnp.bfloat16)
    v_tr = v_f32.T.astype(jnp.bfloat16)
    for h in range(n_group):
        cols = pl.ds(h * HEAD_DIM, HEAD_DIM)
        qr_ref[:, cols] = rope(q_ref[:, cols])
    for h in range(n_group):
        cols = pl.ds(h * HEAD_DIM, HEAD_DIM)
        for blk in range(n_seq // Q_BLK):
            rows = pl.ds(blk * Q_BLK, Q_BLK)
            n_key = (blk + 1) * Q_BLK
            scores = dot_f32(kr_ref[0:n_key, :], qr_ref[rows, cols], NT)
            diag = jnp.where(keep, scores[n_key - Q_BLK:, :], -1e30)
            if blk:
                scores = jnp.concatenate([scores[:n_key - Q_BLK, :], diag], axis=0)
            else:
                scores = diag
            row_max = jnp.max(scores, axis=0, keepdims=True)
            exp_s = jnp.exp2((scores - row_max) * score_mul)
            row_sum = jnp.sum(exp_s, axis=0, keepdims=True)
            probs = (exp_s * (1.0 / row_sum)).astype(jnp.bfloat16)
            o_tr = dot_f32(v_tr[:, :n_key], probs, NN)
            o_ref[rows, cols] = o_tr.T.astype(jnp.bfloat16)
            lse_ref[0, h:h + 1, rows] = row_max * score_mul + jnp.log2(row_sum)


def attn_bwd_kernel(n_group, n_q, n_kv_w, q_ref, k_ref, v_ref, do_ref, lse_ref, cos_ref, sin_ref, d_ref, db_ref, dk_acc, dv_acc):
    n_seq = k_ref.shape[0]
    kv_i = pl.program_id(1)
    cos_t, sin_t = cos_ref[...], sin_ref[...]
    scale = 1.0 / math.sqrt(HEAD_DIM)
    score_mul = LOG2E * scale
    keep = causal_keep(Q_BLK)
    k_tr = k_ref[...].astype(jnp.float32).T.astype(jnp.bfloat16)

    def rope_t(vec_in, rows):
        d_rot = vec_in.astype(jnp.bfloat16).astype(jnp.float32)
        return d_rot * cos_t[rows] - pltpu.roll(d_rot, HEAD_DIM // 2, 1) * sin_t[rows]

    for h in range(n_group):
        cols = pl.ds(h * HEAD_DIM, HEAD_DIM)
        out_cols = pl.ds(pl.multiple_of((kv_i * n_group + h) * HEAD_DIM, HEAD_DIM), HEAD_DIM)
        bias_sum = jnp.zeros((1, HEAD_DIM), jnp.float32)
        for blk in range(n_seq // Q_BLK):
            rows = pl.ds(blk * Q_BLK, Q_BLK)
            n_key = (blk + 1) * Q_BLK
            q_blk, do_blk = q_ref[rows, cols], do_ref[rows, cols]
            scores = dot_f32(k_ref[0:n_key, :], q_blk, NT)
            probs = jnp.exp2(scores * score_mul - lse_ref[0, h:h + 1, rows])
            diag = jnp.where(keep, probs[n_key - Q_BLK:, :], 0.0)
            if blk:
                probs = jnp.concatenate([probs[:n_key - Q_BLK, :], diag], axis=0)
            else:
                probs = diag
            d_probs = dot_f32(v_ref[0:n_key, :], do_blk, NT)
            delta = jnp.sum(probs * d_probs, axis=0, keepdims=True)
            d_scores = (probs * (d_probs - delta) * scale).astype(jnp.bfloat16)
            dv_part = dot_f32(probs.astype(jnp.bfloat16), do_blk, NN)
            dk_part = dot_f32(d_scores, q_blk, NN)
            if h == 0:
                tail = pl.ds(n_key - Q_BLK, Q_BLK)
                if blk:
                    dv_acc[0:n_key - Q_BLK, :] += dv_part[:n_key - Q_BLK, :]
                    dk_acc[0:n_key - Q_BLK, :] += dk_part[:n_key - Q_BLK, :]
                dv_acc[tail, :] = dv_part[n_key - Q_BLK:, :]
                dk_acc[tail, :] = dk_part[n_key - Q_BLK:, :]
            else:
                dv_acc[0:n_key, :] += dv_part
                dk_acc[0:n_key, :] += dk_part
            dq_blk = dot_f32(k_tr[:, :n_key], d_scores, NN).T
            dq_lin = rope_t(dq_blk, slice(blk * Q_BLK, (blk + 1) * Q_BLK))
            bias_sum = bias_sum + jnp.sum(dq_lin, axis=0, keepdims=True)
            d_ref[rows, out_cols] = dq_lin.astype(jnp.bfloat16)
        db_ref[0, :, out_cols] = bias_sum
    dk_lin = rope_t(dk_acc[...], slice(0, n_seq))
    dv_lin = dv_acc[...].astype(jnp.bfloat16)
    k_cols = pl.ds(pl.multiple_of(n_q + kv_i * HEAD_DIM, HEAD_DIM), HEAD_DIM)
    v_cols = pl.ds(pl.multiple_of(n_q + n_kv_w + kv_i * HEAD_DIM, HEAD_DIM), HEAD_DIM)
    d_ref[:, k_cols] = dk_lin.astype(jnp.bfloat16)
    d_ref[:, v_cols] = dv_lin
    db_ref[0, :, k_cols] = jnp.sum(dk_lin, axis=0, keepdims=True)
    db_ref[0, :, v_cols] = jnp.sum(dv_lin.astype(jnp.float32), axis=0, keepdims=True)


def attention_fwd(qkv_lin, cos_t, sin_t, n_batch, n_seq, n_q, n_kv):
    n_tok = n_batch * n_seq
    n_group = n_q // HEAD_DIM // n_kv
    grp_w = n_group * HEAD_DIM
    q_heads = n_q // HEAD_DIM
    flops = 4 * n_tok * n_seq * n_q * 3 // 4
    return pl.pallas_call(
        functools.partial(attn_fwd_kernel, n_group),
        grid=(n_batch, n_kv),
        in_specs=[
            pl.BlockSpec((n_seq, grp_w), lambda b, j: (b, j)),
            pl.BlockSpec((n_seq, HEAD_DIM), lambda b, j: (b, q_heads + j)),
            pl.BlockSpec((n_seq, HEAD_DIM), lambda b, j: (b, q_heads + n_kv + j)),
            pl.BlockSpec((n_seq, HEAD_DIM), lambda b, j: (b, 0)),
            pl.BlockSpec((n_seq, HEAD_DIM), lambda b, j: (b, 0)),
        ],
        out_specs=[
            pl.BlockSpec((n_seq, grp_w), lambda b, j: (b, j)),
            pl.BlockSpec((n_seq, grp_w), lambda b, j: (b, j)),
            pl.BlockSpec((n_seq, HEAD_DIM), lambda b, j: (b, j)),
            pl.BlockSpec((n_seq, HEAD_DIM), lambda b, j: (b, j)),
            pl.BlockSpec((1, 8, n_seq), lambda b, j: (b * n_kv + j, 0, 0)),
        ],
        out_shape=[
            jax.ShapeDtypeStruct((n_tok, n_q), jnp.bfloat16),
            jax.ShapeDtypeStruct((n_tok, n_q), jnp.bfloat16),
            jax.ShapeDtypeStruct((n_tok, n_kv * HEAD_DIM), jnp.bfloat16),
            jax.ShapeDtypeStruct((n_tok, n_kv * HEAD_DIM), jnp.bfloat16),
            jax.ShapeDtypeStruct((n_batch * n_kv, 8, n_seq), jnp.float32),
        ],
        compiler_params=pltpu.CompilerParams(dimension_semantics=('arbitrary', 'arbitrary'), vmem_limit_bytes=48 * 2**20),
        cost_estimate=pl.CostEstimate(flops=flops * 3, bytes_accessed=n_tok * n_q * 10, transcendentals=n_tok * n_seq * q_heads),
        name='attn_fwd',
    )(qkv_lin, qkv_lin, qkv_lin, cos_t, sin_t)


def attention_bwd(q_rot, k_rot, v_bf, d_attn, lse, cos_t, sin_t, n_batch, n_seq, n_kv):
    n_tok, n_q = q_rot.shape
    n_group = n_q // HEAD_DIM // n_kv
    grp_w = n_group * HEAD_DIM
    n_kv_w = n_kv * HEAD_DIM
    n_all = n_q + 2 * n_kv_w
    flops = 10 * n_tok * n_seq * n_q * 3 // 4
    return pl.pallas_call(
        functools.partial(attn_bwd_kernel, n_group, n_q, n_kv_w),
        grid=(n_batch, n_kv),
        in_specs=[
            pl.BlockSpec((n_seq, grp_w), lambda b, j: (b, j)),
            pl.BlockSpec((n_seq, HEAD_DIM), lambda b, j: (b, j)),
            pl.BlockSpec((n_seq, HEAD_DIM), lambda b, j: (b, j)),
            pl.BlockSpec((n_seq, grp_w), lambda b, j: (b, j)),
            pl.BlockSpec((1, 8, n_seq), lambda b, j: (b * n_kv + j, 0, 0)),
            pl.BlockSpec((n_seq, HEAD_DIM), lambda b, j: (b, 0)),
            pl.BlockSpec((n_seq, HEAD_DIM), lambda b, j: (b, 0)),
        ],
        out_specs=[
            pl.BlockSpec((n_seq, n_all), lambda b, j: (b, 0)),
            pl.BlockSpec((1, 1, n_all), lambda b, j: (b, 0, 0)),
        ],
        out_shape=[
            jax.ShapeDtypeStruct((n_tok, n_all), jnp.bfloat16),
            jax.ShapeDtypeStruct((n_batch, 1, n_all), jnp.float32),
        ],
        scratch_shapes=[pltpu.VMEM((n_seq, HEAD_DIM), jnp.float32), pltpu.VMEM((n_seq, HEAD_DIM), jnp.float32)],
        compiler_params=pltpu.CompilerParams(dimension_semantics=('arbitrary', 'arbitrary'), vmem_limit_bytes=48 * 2**20),
        cost_estimate=pl.CostEstimate(flops=flops * 3, bytes_accessed=n_tok * n_q * 8, transcendentals=n_tok * n_seq * n_q // HEAD_DIM),
        name='attn_bwd',
    )(q_rot, k_rot, v_bf, d_attn, lse, cos_t, sin_t)


def inv_rms_of(hidden):
    x_f32 = hidden.astype(jnp.float32)
    return lax.rsqrt(jnp.mean(x_f32 * x_f32, axis=-1, keepdims=True) + NORM_EPS)


def norm_apply(hidden, inv_rms, gain_vec):
    return (hidden.astype(jnp.float32) * inv_rms * gain_vec.astype(jnp.float32)).astype(jnp.bfloat16)


def norm_bwd(hidden, inv_rms, gain_vec, d_normed):
    unit_rows = hidden.astype(jnp.float32) * inv_rms
    d_gain = jnp.sum(d_normed * unit_rows, axis=0)
    d_unit = d_normed * gain_vec.astype(jnp.float32)
    d_hidden = inv_rms * (d_unit - unit_rows * jnp.mean(d_unit * unit_rows, axis=-1, keepdims=True))
    return d_hidden, d_gain


def gather_rows(shard):
    return lax.all_gather(shard, FSDP_AXIS, axis=0, tiled=True)


def scatter_rows(grad_part):
    return lax.psum_scatter(grad_part, FSDP_AXIS, scatter_dimension=0, tiled=True)


def after(value, *earlier):
    return lax.optimization_barrier((value,) + earlier)[0]


def solution(mesh):
    act_spec = P(FSDP_AXIS, None, None)
    mat_spec = P(FSDP_AXIS, None)
    vec_spec = P(FSDP_AXIS)
    param_specs = (vec_spec, mat_spec, vec_spec, mat_spec, vec_spec, mat_spec, vec_spec, mat_spec, vec_spec, mat_spec, mat_spec, mat_spec)
    in_specs_all = (act_spec, act_spec, mat_spec) + param_specs
    out_specs_all = (act_spec, act_spec) + param_specs
    n_dev = mesh.shape[FSDP_AXIS]

    def local_step(hidden3, grad_out3, positions, *shards):
        s_gain_attn, s_wq, s_bq, s_wk, s_bk, s_wv, s_bv, s_wo, s_gain_mlp, s_gate, s_up, s_down = shards
        n_batch, n_seq, n_model = hidden3.shape
        n_tok = n_batch * n_seq
        hidden = hidden3.reshape(n_tok, n_model)
        grad_out = grad_out3.reshape(n_tok, n_model)
        n_rows, n_q = s_wq.shape
        n_kv_w = s_wk.shape[1]
        n_kv = n_kv_w // HEAD_DIM
        n_all = n_q + 2 * n_kv_w

        def column(vec):
            return jnp.pad(vec, (0, n_rows - vec.shape[0]))[:, None]

        small = jnp.concatenate([column(s_gain_attn), column(s_gain_mlp), column(s_bq), column(s_bk), column(s_bv), jnp.zeros((n_rows, 123), jnp.bfloat16)], axis=1)
        packed = gather_rows(jnp.concatenate([s_wq, s_wk, s_wv, small], axis=1))
        w_qkv = packed[:, :n_all]
        vecs = packed[:, n_all:n_all + 5]
        gain_attn, gain_mlp, b_q = vecs[:, 0], vecs[:, 1], vecs[:, 2]
        kv_rows = vecs.reshape(n_dev, n_rows, 5)[:, :n_kv_w // n_dev, :]
        b_k, b_v = kv_rows[:, :, 3].reshape(n_kv_w), kv_rows[:, :, 4].reshape(n_kv_w)
        b_qkv = jnp.concatenate([b_q, b_k, b_v]).astype(jnp.float32)
        w_o = gather_rows(s_wo)
        w_gate, w_up, w_down = gather_rows(s_gate), gather_rows(s_up), gather_rows(s_down)

        cos_t, sin_t = rope_tables(positions)
        inv_attn = inv_rms_of(hidden)
        normed_attn = norm_apply(hidden, inv_attn, gain_attn)
        qkv_lin = matmul_f32('td,de->te', normed_attn, w_qkv) + b_qkv
        attn_out, q_rot, k_rot, v_bf, lse = attention_fwd(qkv_lin, cos_t, sin_t, n_batch, n_seq, n_q, n_kv)
        resid_mid = (hidden.astype(jnp.float32) + matmul_f32('te,ed->td', attn_out, w_o)).astype(jnp.bfloat16)
        inv_mlp = inv_rms_of(resid_mid)
        normed_mlp = norm_apply(resid_mid, inv_mlp, gain_mlp)
        gate_pre = matmul_f32('td,df->tf', normed_mlp, w_gate)
        up_proj = matmul_f32('td,df->tf', normed_mlp, w_up)
        act_mlp = (jax.nn.silu(gate_pre) * up_proj).astype(jnp.bfloat16)

        d_w_down = matmul_f32('tf,td->fd', act_mlp, grad_out)
        g_down = scatter_rows(d_w_down)
        grad_out_b = after(grad_out, d_w_down)
        d_act = matmul_f32('td,fd->tf', grad_out_b, w_down).astype(jnp.bfloat16).astype(jnp.float32)
        gate_sig = jax.nn.sigmoid(gate_pre)
        d_gate = (d_act * up_proj * gate_sig * (1.0 + gate_pre * (1.0 - gate_sig))).astype(jnp.bfloat16)
        d_up = (d_act * gate_pre * gate_sig).astype(jnp.bfloat16)
        d_w_gate = matmul_f32('td,tf->df', normed_mlp, d_gate)
        g_gate = scatter_rows(d_w_gate)
        d_w_up = matmul_f32('td,tf->df', after(normed_mlp, d_w_gate), d_up)
        g_up = scatter_rows(d_w_up)
        d_gate_b, d_up_b = lax.optimization_barrier((d_gate, d_up, d_w_up))[:2]
        d_normed_mlp = (matmul_f32('tf,df->td', d_gate_b, w_gate) + matmul_f32('tf,df->td', d_up_b, w_up)).astype(jnp.bfloat16).astype(jnp.float32)
        d_resid_norm, d_gain_mlp = norm_bwd(resid_mid, inv_mlp, gain_mlp, d_normed_mlp)
        d_resid = (grad_out.astype(jnp.float32) + d_resid_norm).astype(jnp.bfloat16)
        d_w_o = matmul_f32('te,td->ed', attn_out, d_resid)
        g_o = scatter_rows(d_w_o)
        d_attn = matmul_f32('td,ed->te', after(d_resid, d_w_o), w_o).astype(jnp.bfloat16)
        d_qkv, d_bias_rows = attention_bwd(q_rot, k_rot, v_bf, d_attn, lse, cos_t, sin_t, n_batch, n_seq, n_kv)
        d_w_qkv = matmul_f32('td,te->de', normed_attn, d_qkv)
        g_qkv = scatter_rows(d_w_qkv)
        d_qkv_b, act_last = lax.optimization_barrier((d_qkv, act_mlp, d_w_qkv))[:2]
        d_normed_attn = matmul_f32('te,de->td', d_qkv_b, w_qkv).astype(jnp.bfloat16).astype(jnp.float32)
        d_hidden_norm, d_gain_attn = norm_bwd(hidden, inv_attn, gain_attn, d_normed_attn)
        grad_hidden = (d_resid.astype(jnp.float32) + d_hidden_norm).astype(jnp.bfloat16)
        layer_out = (resid_mid.astype(jnp.float32) + matmul_f32('tf,fd->td', act_last, w_down)).astype(jnp.bfloat16)

        d_bias = jnp.sum(d_bias_rows, axis=(0, 1))
        g_gain_attn, g_gain_mlp = scatter_rows(d_gain_attn), scatter_rows(d_gain_mlp)
        g_bq = scatter_rows(d_bias[:n_q])
        g_bk, g_bv = scatter_rows(d_bias[n_q:n_q + n_kv_w]), scatter_rows(d_bias[n_q + n_kv_w:])
        g_wq, g_wk, g_wv = g_qkv[:, :n_q], g_qkv[:, n_q:n_q + n_kv_w], g_qkv[:, n_q + n_kv_w:]
        return (layer_out.reshape(hidden3.shape), grad_hidden.reshape(hidden3.shape), g_gain_attn, g_wq, g_bq, g_wk, g_bk, g_wv, g_bv, g_o, g_gain_mlp, g_gate, g_up, g_down)


    return jax.shard_map(local_step, mesh=mesh, in_specs=in_specs_all, out_specs=out_specs_all, check_vma=False)
```

```python
import functools
import math
import jax
import jax.numpy as jnp
from jax import lax
from jax.experimental import pallas as pl
from jax.experimental.pallas import tpu as pltpu
from jax.sharding import PartitionSpec as P

HEAD_DIM = 128
NORM_EPS = 1e-6
ROPE_THETA = 1000000.0
FSDP_AXIS = 'fsdp'
LOG2E = 1.4426950408889634
Q_BLK = 256
NT = (((1,), (1,)), ((), ()))
NN = (((1,), (0,)), ((), ()))


def matmul_f32(eq_form, lhs_arr, rhs_arr):
    return jnp.einsum(eq_form, lhs_arr, rhs_arr, preferred_element_type=jnp.float32)


def dot_f32(lhs_arr, rhs_arr, dims):
    return lax.dot_general(lhs_arr, rhs_arr, dims, preferred_element_type=jnp.float32)


def rope_tables(positions):
    inv_freq = 1.0 / jnp.power(ROPE_THETA, jnp.arange(0, HEAD_DIM, 2).astype(jnp.float32) / HEAD_DIM)
    angles = positions.astype(jnp.float32).reshape(-1, 1) * inv_freq
    cos_h, sin_h = jnp.cos(angles), jnp.sin(angles)
    return jnp.concatenate([cos_h, cos_h], axis=-1), jnp.concatenate([-sin_h, sin_h], axis=-1)


def causal_keep(n_blk):
    key_i = lax.broadcasted_iota(jnp.int32, (n_blk, n_blk), 0)
    qry_i = lax.broadcasted_iota(jnp.int32, (n_blk, n_blk), 1)
    return key_i <= qry_i


def attn_fwd_kernel(n_group, q_ref, k_ref, v_ref, cos_ref, sin_ref, o_ref, qr_ref, kr_ref, vb_ref, lse_ref):
    n_seq = k_ref.shape[0]
    cos_t, sin_t = cos_ref[...], sin_ref[...]
    score_mul = LOG2E / math.sqrt(HEAD_DIM)
    keep = causal_keep(Q_BLK)

    def rope(vec_in):
        return (vec_in * cos_t + pltpu.roll(vec_in, HEAD_DIM // 2, 1) * sin_t).astype(jnp.bfloat16)

    kr_ref[...] = rope(k_ref[...])
    v_f32 = v_ref[...].astype(jnp.bfloat16).astype(jnp.float32)
    vb_ref[...] = v_f32.astype(jnp.bfloat16)
    v_tr = v_f32.T.astype(jnp.bfloat16)
    for h in range(n_group):
        cols = pl.ds(h * HEAD_DIM, HEAD_DIM)
        qr_ref[:, cols] = rope(q_ref[:, cols])
    for h in range(n_group):
        cols = pl.ds(h * HEAD_DIM, HEAD_DIM)
        for blk in range(n_seq // Q_BLK):
            rows = pl.ds(blk * Q_BLK, Q_BLK)
            n_key = (blk + 1) * Q_BLK
            scores = dot_f32(kr_ref[0:n_key, :], qr_ref[rows, cols], NT)
            diag = jnp.where(keep, scores[n_key - Q_BLK:, :], -1e30)
            if blk:
                scores = jnp.concatenate([scores[:n_key - Q_BLK, :], diag], axis=0)
            else:
                scores = diag
            row_max = jnp.max(scores, axis=0, keepdims=True)
            exp_s = jnp.exp2((scores - row_max) * score_mul)
            row_sum = jnp.sum(exp_s, axis=0, keepdims=True)
            probs = (exp_s * (1.0 / row_sum)).astype(jnp.bfloat16)
            o_tr = dot_f32(v_tr[:, :n_key], probs, NN)
            o_ref[rows, cols] = o_tr.T.astype(jnp.bfloat16)
            lse_ref[0, h:h + 1, rows] = row_max * score_mul + jnp.log2(row_sum)


def attn_bwd_kernel(n_group, n_q, n_kv_w, q_ref, k_ref, v_ref, do_ref, lse_ref, cos_ref, sin_ref, d_ref, db_ref, dk_acc, dv_acc):
    n_seq = k_ref.shape[0]
    kv_i = pl.program_id(1)
    cos_t, sin_t = cos_ref[...], sin_ref[...]
    scale = 1.0 / math.sqrt(HEAD_DIM)
    score_mul = LOG2E * scale
    keep = causal_keep(Q_BLK)
    k_tr = k_ref[...].astype(jnp.float32).T.astype(jnp.bfloat16)

    def rope_t(vec_in, rows):
        d_rot = vec_in.astype(jnp.bfloat16).astype(jnp.float32)
        return d_rot * cos_t[rows] - pltpu.roll(d_rot, HEAD_DIM // 2, 1) * sin_t[rows]

    for h in range(n_group):
        cols = pl.ds(h * HEAD_DIM, HEAD_DIM)
        out_cols = pl.ds(pl.multiple_of((kv_i * n_group + h) * HEAD_DIM, HEAD_DIM), HEAD_DIM)
        bias_sum = jnp.zeros((1, HEAD_DIM), jnp.float32)
        for blk in range(n_seq // Q_BLK):
            rows = pl.ds(blk * Q_BLK, Q_BLK)
            n_key = (blk + 1) * Q_BLK
            q_blk, do_blk = q_ref[rows, cols], do_ref[rows, cols]
            scores = dot_f32(k_ref[0:n_key, :], q_blk, NT)
            probs = jnp.exp2(scores * score_mul - lse_ref[0, h:h + 1, rows])
            diag = jnp.where(keep, probs[n_key - Q_BLK:, :], 0.0)
            if blk:
                probs = jnp.concatenate([probs[:n_key - Q_BLK, :], diag], axis=0)
            else:
                probs = diag
            d_probs = dot_f32(v_ref[0:n_key, :], do_blk, NT)
            delta = jnp.sum(probs * d_probs, axis=0, keepdims=True)
            d_scores = (probs * (d_probs - delta) * scale).astype(jnp.bfloat16)
            dv_part = dot_f32(probs.astype(jnp.bfloat16), do_blk, NN)
            dk_part = dot_f32(d_scores, q_blk, NN)
            if h == 0:
                tail = pl.ds(n_key - Q_BLK, Q_BLK)
                if blk:
                    dv_acc[0:n_key - Q_BLK, :] += dv_part[:n_key - Q_BLK, :]
                    dk_acc[0:n_key - Q_BLK, :] += dk_part[:n_key - Q_BLK, :]
                dv_acc[tail, :] = dv_part[n_key - Q_BLK:, :]
                dk_acc[tail, :] = dk_part[n_key - Q_BLK:, :]
            else:
                dv_acc[0:n_key, :] += dv_part
                dk_acc[0:n_key, :] += dk_part
            dq_blk = dot_f32(k_tr[:, :n_key], d_scores, NN).T
            dq_lin = rope_t(dq_blk, slice(blk * Q_BLK, (blk + 1) * Q_BLK))
            bias_sum = bias_sum + jnp.sum(dq_lin, axis=0, keepdims=True)
            d_ref[rows, out_cols] = dq_lin.astype(jnp.bfloat16)
        db_ref[0, :, out_cols] = bias_sum
    dk_lin = rope_t(dk_acc[...], slice(0, n_seq))
    dv_lin = dv_acc[...].astype(jnp.bfloat16)
    k_cols = pl.ds(pl.multiple_of(n_q + kv_i * HEAD_DIM, HEAD_DIM), HEAD_DIM)
    v_cols = pl.ds(pl.multiple_of(n_q + n_kv_w + kv_i * HEAD_DIM, HEAD_DIM), HEAD_DIM)
    d_ref[:, k_cols] = dk_lin.astype(jnp.bfloat16)
    d_ref[:, v_cols] = dv_lin
    db_ref[0, :, k_cols] = jnp.sum(dk_lin, axis=0, keepdims=True)
    db_ref[0, :, v_cols] = jnp.sum(dv_lin.astype(jnp.float32), axis=0, keepdims=True)


def attention_fwd(qkv_lin, cos_t, sin_t, n_batch, n_seq, n_q, n_kv):
    n_tok = n_batch * n_seq
    n_group = n_q // HEAD_DIM // n_kv
    grp_w = n_group * HEAD_DIM
    q_heads = n_q // HEAD_DIM
    flops = 4 * n_tok * n_seq * n_q * 3 // 4
    return pl.pallas_call(
        functools.partial(attn_fwd_kernel, n_group),
        grid=(n_batch, n_kv),
        in_specs=[
            pl.BlockSpec((n_seq, grp_w), lambda b, j: (b, j)),
            pl.BlockSpec((n_seq, HEAD_DIM), lambda b, j: (b, q_heads + j)),
            pl.BlockSpec((n_seq, HEAD_DIM), lambda b, j: (b, q_heads + n_kv + j)),
            pl.BlockSpec((n_seq, HEAD_DIM), lambda b, j: (b, 0)),
            pl.BlockSpec((n_seq, HEAD_DIM), lambda b, j: (b, 0)),
        ],
        out_specs=[
            pl.BlockSpec((n_seq, grp_w), lambda b, j: (b, j)),
            pl.BlockSpec((n_seq, grp_w), lambda b, j: (b, j)),
            pl.BlockSpec((n_seq, HEAD_DIM), lambda b, j: (b, j)),
            pl.BlockSpec((n_seq, HEAD_DIM), lambda b, j: (b, j)),
            pl.BlockSpec((1, 8, n_seq), lambda b, j: (b * n_kv + j, 0, 0)),
        ],
        out_shape=[
            jax.ShapeDtypeStruct((n_tok, n_q), jnp.bfloat16),
            jax.ShapeDtypeStruct((n_tok, n_q), jnp.bfloat16),
            jax.ShapeDtypeStruct((n_tok, n_kv * HEAD_DIM), jnp.bfloat16),
            jax.ShapeDtypeStruct((n_tok, n_kv * HEAD_DIM), jnp.bfloat16),
            jax.ShapeDtypeStruct((n_batch * n_kv, 8, n_seq), jnp.float32),
        ],
        compiler_params=pltpu.CompilerParams(dimension_semantics=('arbitrary', 'arbitrary'), vmem_limit_bytes=48 * 2**20),
        cost_estimate=pl.CostEstimate(flops=flops * 3, bytes_accessed=n_tok * n_q * 10, transcendentals=n_tok * n_seq * q_heads),
        name='attn_fwd',
    )(qkv_lin, qkv_lin, qkv_lin, cos_t, sin_t)


def attention_bwd(q_rot, k_rot, v_bf, d_attn, lse, cos_t, sin_t, n_batch, n_seq, n_kv):
    n_tok, n_q = q_rot.shape
    n_group = n_q // HEAD_DIM // n_kv
    grp_w = n_group * HEAD_DIM
    n_kv_w = n_kv * HEAD_DIM
    n_all = n_q + 2 * n_kv_w
    flops = 10 * n_tok * n_seq * n_q * 3 // 4
    return pl.pallas_call(
        functools.partial(attn_bwd_kernel, n_group, n_q, n_kv_w),
        grid=(n_batch, n_kv),
        in_specs=[
            pl.BlockSpec((n_seq, grp_w), lambda b, j: (b, j)),
            pl.BlockSpec((n_seq, HEAD_DIM), lambda b, j: (b, j)),
            pl.BlockSpec((n_seq, HEAD_DIM), lambda b, j: (b, j)),
            pl.BlockSpec((n_seq, grp_w), lambda b, j: (b, j)),
            pl.BlockSpec((1, 8, n_seq), lambda b, j: (b * n_kv + j, 0, 0)),
            pl.BlockSpec((n_seq, HEAD_DIM), lambda b, j: (b, 0)),
            pl.BlockSpec((n_seq, HEAD_DIM), lambda b, j: (b, 0)),
        ],
        out_specs=[
            pl.BlockSpec((n_seq, n_all), lambda b, j: (b, 0)),
            pl.BlockSpec((1, 1, n_all), lambda b, j: (b, 0, 0)),
        ],
        out_shape=[
            jax.ShapeDtypeStruct((n_tok, n_all), jnp.bfloat16),
            jax.ShapeDtypeStruct((n_batch, 1, n_all), jnp.float32),
        ],
        scratch_shapes=[pltpu.VMEM((n_seq, HEAD_DIM), jnp.float32), pltpu.VMEM((n_seq, HEAD_DIM), jnp.float32)],
        compiler_params=pltpu.CompilerParams(dimension_semantics=('arbitrary', 'arbitrary'), vmem_limit_bytes=48 * 2**20),
        cost_estimate=pl.CostEstimate(flops=flops * 3, bytes_accessed=n_tok * n_q * 8, transcendentals=n_tok * n_seq * n_q // HEAD_DIM),
        name='attn_bwd',
    )(q_rot, k_rot, v_bf, d_attn, lse, cos_t, sin_t)


def inv_rms_of(hidden):
    x_f32 = hidden.astype(jnp.float32)
    return lax.rsqrt(jnp.mean(x_f32 * x_f32, axis=-1, keepdims=True) + NORM_EPS)


def norm_apply(hidden, inv_rms, gain_vec):
    return (hidden.astype(jnp.float32) * inv_rms * gain_vec.astype(jnp.float32)).astype(jnp.bfloat16)


def norm_bwd(hidden, inv_rms, gain_vec, d_normed):
    unit_rows = hidden.astype(jnp.float32) * inv_rms
    d_gain = jnp.sum(d_normed * unit_rows, axis=0)
    d_unit = d_normed * gain_vec.astype(jnp.float32)
    d_hidden = inv_rms * (d_unit - unit_rows * jnp.mean(d_unit * unit_rows, axis=-1, keepdims=True))
    return d_hidden, d_gain


def gather_rows(shard):
    return lax.all_gather(shard, FSDP_AXIS, axis=0, tiled=True)


def scatter_rows(grad_part):
    return lax.psum_scatter(grad_part, FSDP_AXIS, scatter_dimension=0, tiled=True)


def after(value, *earlier):
    return lax.optimization_barrier((value,) + earlier)[0]


def solution(mesh):
    act_spec = P(FSDP_AXIS, None, None)
    mat_spec = P(FSDP_AXIS, None)
    vec_spec = P(FSDP_AXIS)
    param_specs = (vec_spec, mat_spec, vec_spec, mat_spec, vec_spec, mat_spec, vec_spec, mat_spec, vec_spec, mat_spec, mat_spec, mat_spec)
    in_specs_all = (act_spec, act_spec, mat_spec) + param_specs
    out_specs_all = (act_spec, act_spec) + param_specs
    n_dev = mesh.shape[FSDP_AXIS]

    def local_step(hidden3, grad_out3, positions, *shards):
        s_gain_attn, s_wq, s_bq, s_wk, s_bk, s_wv, s_bv, s_wo, s_gain_mlp, s_gate, s_up, s_down = shards
        n_batch, n_seq, n_model = hidden3.shape
        n_tok = n_batch * n_seq
        hidden = hidden3.reshape(n_tok, n_model)
        grad_out = grad_out3.reshape(n_tok, n_model)
        n_rows, n_q = s_wq.shape
        n_kv_w = s_wk.shape[1]
        n_kv = n_kv_w // HEAD_DIM
        n_all = n_q + 2 * n_kv_w

        def column(vec):
            return jnp.pad(vec, (0, n_rows - vec.shape[0]))[:, None]

        small = jnp.concatenate([column(s_gain_attn), column(s_gain_mlp), column(s_bq), column(s_bk), column(s_bv), jnp.zeros((n_rows, 123), jnp.bfloat16)], axis=1)
        packed = gather_rows(jnp.concatenate([s_wq, s_wk, s_wv, small], axis=1))
        w_qkv = packed[:, :n_all]
        vecs = packed[:, n_all:n_all + 5]
        gain_attn, gain_mlp, b_q = vecs[:, 0], vecs[:, 1], vecs[:, 2]
        kv_rows = vecs.reshape(n_dev, n_rows, 5)[:, :n_kv_w // n_dev, :]
        b_k, b_v = kv_rows[:, :, 3].reshape(n_kv_w), kv_rows[:, :, 4].reshape(n_kv_w)
        b_qkv = jnp.concatenate([b_q, b_k, b_v]).astype(jnp.float32)
        w_o = gather_rows(s_wo)
        w_gate, w_up, w_down = gather_rows(s_gate), gather_rows(s_up), gather_rows(s_down)

        cos_t, sin_t = rope_tables(positions)
        inv_attn = inv_rms_of(hidden)
        normed_attn = norm_apply(hidden, inv_attn, gain_attn)
        qkv_lin = matmul_f32('td,de->te', normed_attn, w_qkv) + b_qkv
        attn_out, q_rot, k_rot, v_bf, lse = attention_fwd(qkv_lin, cos_t, sin_t, n_batch, n_seq, n_q, n_kv)
        resid_mid = (hidden.astype(jnp.float32) + matmul_f32('te,ed->td', attn_out, w_o)).astype(jnp.bfloat16)
        inv_mlp = inv_rms_of(resid_mid)
        normed_mlp = norm_apply(resid_mid, inv_mlp, gain_mlp)
        gate_pre = matmul_f32('td,df->tf', normed_mlp, w_gate)
        up_proj = matmul_f32('td,df->tf', normed_mlp, w_up)
        act_mlp = (jax.nn.silu(gate_pre) * up_proj).astype(jnp.bfloat16)

        d_w_down = matmul_f32('tf,td->fd', act_mlp, grad_out)
        g_down = scatter_rows(d_w_down)
        grad_out_b = after(grad_out, d_w_down)
        d_act = matmul_f32('td,fd->tf', grad_out_b, w_down).astype(jnp.bfloat16).astype(jnp.float32)
        gate_sig = jax.nn.sigmoid(gate_pre)
        d_gate = (d_act * up_proj * gate_sig * (1.0 + gate_pre * (1.0 - gate_sig))).astype(jnp.bfloat16)
        d_up = (d_act * gate_pre * gate_sig).astype(jnp.bfloat16)
        d_w_gate = matmul_f32('td,tf->df', normed_mlp, d_gate)
        g_gate = scatter_rows(d_w_gate)
        d_w_up = matmul_f32('td,tf->df', after(normed_mlp, d_w_gate), d_up)
        g_up = scatter_rows(d_w_up)
        d_gate_b, d_up_b = lax.optimization_barrier((d_gate, d_up, d_w_up))[:2]
        d_normed_mlp = (matmul_f32('tf,df->td', d_gate_b, w_gate) + matmul_f32('tf,df->td', d_up_b, w_up)).astype(jnp.bfloat16).astype(jnp.float32)
        d_resid_norm, d_gain_mlp = norm_bwd(resid_mid, inv_mlp, gain_mlp, d_normed_mlp)
        d_resid = (grad_out.astype(jnp.float32) + d_resid_norm).astype(jnp.bfloat16)
        d_w_o = matmul_f32('te,td->ed', attn_out, d_resid)
        g_o = scatter_rows(d_w_o)
        d_attn = matmul_f32('td,ed->te', after(d_resid, d_w_o), w_o).astype(jnp.bfloat16)
        d_qkv, d_bias_rows = attention_bwd(q_rot, k_rot, v_bf, d_attn, lse, cos_t, sin_t, n_batch, n_seq, n_kv)
        d_w_qkv = matmul_f32('td,te->de', normed_attn, d_qkv)
        g_qkv = scatter_rows(d_w_qkv)
        d_qkv_b, act_last = lax.optimization_barrier((d_qkv, act_mlp, d_w_qkv))[:2]
        d_normed_attn = matmul_f32('te,de->td', d_qkv_b, w_qkv).astype(jnp.bfloat16).astype(jnp.float32)
        d_hidden_norm, d_gain_attn = norm_bwd(hidden, inv_attn, gain_attn, d_normed_attn)
        grad_hidden = (d_resid.astype(jnp.float32) + d_hidden_norm).astype(jnp.bfloat16)
        layer_out = (resid_mid.astype(jnp.float32) + matmul_f32('tf,fd->td', act_last, w_down)).astype(jnp.bfloat16)

        d_bias = jnp.sum(d_bias_rows, axis=(0, 1))
        kv_shard = n_kv_w // n_dev

        def kv_column(vec):
            return jnp.pad(vec.reshape(n_dev, kv_shard), ((0, 0), (0, n_rows - kv_shard))).reshape(n_model)

        vec_rows = jnp.stack([d_gain_attn, d_gain_mlp, d_bias[:n_q], kv_column(d_bias[n_q:n_q + n_kv_w]), kv_column(d_bias[n_q + n_kv_w:])])
        vec_rows = jnp.pad(vec_rows, ((0, 3), (0, 0))).reshape(8, n_dev, n_rows).transpose(1, 0, 2)
        vec_rows = jnp.pad(vec_rows, ((0, 0), (0, 0), (0, 256 - n_rows))).reshape(n_dev * 8, 256)
        g_vecs = scatter_rows(vec_rows)
        g_gain_attn, g_gain_mlp, g_bq = g_vecs[0, :n_rows], g_vecs[1, :n_rows], g_vecs[2, :n_rows]
        g_bk, g_bv = g_vecs[3, :kv_shard], g_vecs[4, :kv_shard]
        g_wq, g_wk, g_wv = g_qkv[:, :n_q], g_qkv[:, n_q:n_q + n_kv_w], g_qkv[:, n_q + n_kv_w:]
        return (layer_out.reshape(hidden3.shape), grad_hidden.reshape(hidden3.shape), g_gain_attn, g_wq, g_bq, g_wk, g_bk, g_wv, g_bv, g_o, g_gain_mlp, g_gate, g_up, g_down)


    return jax.shard_map(local_step, mesh=mesh, in_specs=in_specs_all, out_specs=out_specs_all, check_vma=False)
```
